256 devices in a mesh: groups: 4 (over y, x), dom: 64 (over z, core).
Axes of the slice: x: 2, y: 2, z: 32, core: 2. Of those that a mesh axis runs over, the one named last changes fastest.
The devices are a block of a 4x8x32 slice.
Arguments:
- particles: bfloat16 [8192, 4096], P(('groups', 'dom')), parts along dimension 0, may hold values from -5 to 5
- dataset: bfloat16 [16384, 4096], P(('groups', 'dom')), parts along dimension 0, may hold values from -0.09375 to 0.09375
- labels: int32 [16384], P(('groups', 'dom')), parts along dimension 0, may hold values 0 or 1
- batch_index: int32 [4096], P(('groups', 'dom')), parts along dimension 0, may hold values from 0 to 4095, as said below
Outputs:
- driving: float32 [8192, 4096], P(('groups', 'dom')), parts along dimension 0
- spreading: float32 [8192, 4096], P(('groups', 'dom')), parts along dimension 0
The draws below stay inside these ranges and needn't reach their ends.
There are 4 independent parts, one for each index of `groups`. The reference program is written for one: setup_inputs(seed, part) draws one part's arguments, and reference() takes and returns one part's arrays. A program takes and returns all parts, laid end to end along the dimension named above; each array names one. Nothing has to cross between parts.
Inputs may be any that keep to these rules, and one draw needn't show every extreme that they name: `batch_index`: entry b names a row of block b // 16 of the dataset, that is a row from (b // 16) * 64 to (b // 16 + 1) * 64 - 1; rows may repeat.
All inputs are finite; a program needn't handle non-finite values. No bound on the sum of `labels` on one device may be relied on, other than what follows from the above.
Results may differ from the reference program's by a relative error of at most 0.0003.
Values may be sent and summed in bfloat16 or wider, within the bound.
A program may use at most 128 MiB of HBM per device.

```python
import jax
import jax.numpy as jnp
from jax import lax

D = 4096
BATCH_DEV = 16
DATA_DEV = 64
NP = 2048
BATCH = 1024
DATA = 4096


def draw_particles(key, part):
    key_centre = jax.random.fold_in(key, 11)
    key_radius = jax.random.fold_in(key, 12)
    key_noise = jax.random.fold_in(key, 13)
    key_directions = jax.random.fold_in(key, 14)
    key_latent = jax.random.fold_in(key, 15)
    centre = 0.5 * jnp.clip(jax.random.normal(key_centre, (D,), jnp.float32), -4.0, 4.0)
    radii = jnp.exp(jax.random.uniform(key_radius, (NP, 1), jnp.float32, jnp.log(0.1), jnp.log(0.3)))
    directions = jax.random.normal(key_directions, (8, D), jnp.float32) / jnp.sqrt(jnp.float32(D))
    spread = jnp.sqrt(jnp.float32(0.0390625 * D))
    noise = jnp.clip(jax.random.normal(key_noise, (NP, D), jnp.float32), -4.0, 4.0)
    latent = spread * jnp.clip(jax.random.normal(key_latent, (NP, 8), jnp.float32), -4.0, 4.0)
    placed = jnp.dot(latent, directions)
    field = centre[None, :] + placed + radii * noise
    return jnp.clip(field, -5.0, 5.0).astype(jnp.bfloat16)


def draw_batch_index(key, part):
    block = jnp.arange(BATCH, dtype=jnp.int32) // BATCH_DEV
    offset = jax.random.randint(jax.random.fold_in(key, 21), (BATCH,), 0, DATA_DEV, jnp.int32)
    return (block * DATA_DEV + offset).astype(jnp.int32)


def place_ends(drawn, stream_key, least, top_value):
    longest = drawn.shape.index(max(drawn.shape))
    spots = []
    for shift in (0, 1):
        where = [jax.random.randint(jax.random.fold_in(stream_key, axis), (), 0, length) for axis, length in enumerate(drawn.shape)]
        where[longest] = (where[longest] + shift) % drawn.shape[longest]
        spots.append(tuple(where))
    return drawn.at[spots[0]].set(least).at[spots[1]].set(top_value)


def level_of(stream_key, shape, cuts, low, top_value):
    level, own = 1.0, jax.random.fold_in(stream_key, 6)
    for dim, parts in cuts:
        steps = jnp.exp(jax.random.uniform(jax.random.fold_in(own, dim), (parts,), jnp.float32, low / len(cuts), top_value / len(cuts)))
        level = level * jnp.repeat(steps, shape[dim] // parts).reshape([-1 if axis == dim else 1 for axis in range(len(shape))])
    return level


def normal_values(stream_key, extent, width, bound, cuts=(), held_as=jnp.bfloat16):
    level = level_of(stream_key, extent, cuts, -0.22, 0.18) if cuts else 1.0
    array = jax.random.normal(stream_key, extent, jnp.float32) * width * level
    return jnp.minimum(jnp.maximum(array, -bound), bound).astype(held_as)


def setup_inputs(seed: int = 0, part: int = 0) -> dict:
    key_list = jax.random.split(jax.random.key(seed), 5)
    part_splits = jax.random.split(jax.random.fold_in(key_list[4], part), 5)
    return {
        "particles": draw_particles(jax.random.fold_in(jax.random.fold_in(key_list[4], part), 71), part),
        "dataset": normal_values(part_splits[1], (DATA, D), D ** -0.5, 0.09375, ((0, 64),)),
        "labels": place_ends((jax.random.randint(part_splits[2], (DATA,), 0, 2) < 1).astype(jnp.int32), jax.random.fold_in(part_splits[2], 1), 0, 1),
        "batch_index": draw_batch_index(jax.random.fold_in(jax.random.fold_in(key_list[4], part), 71), part),
    }


prior_precision = 1.0


def reference(particles, dataset, labels, batch_index):
    rows = jnp.take(dataset, batch_index, axis=0)
    targets = jnp.take(labels, batch_index).astype(jnp.float32)
    particles_f = particles.astype(jnp.float32)
    logits = lax.dot_general(particles, rows, (((1,), (1,)), ((), ())), preferred_element_type=jnp.float32)
    misfit = (targets[None, :] - jax.nn.sigmoid(logits)).astype(jnp.bfloat16)
    pulled = jnp.dot(misfit, rows, preferred_element_type=jnp.float32)
    scores = (-prior_precision * particles_f + (DATA / BATCH) * pulled).astype(jnp.bfloat16)
    squares = jnp.sum(particles_f * particles_f, axis=1)
    cross = lax.dot_general(particles, particles, (((1,), (1,)), ((), ())), preferred_element_type=jnp.float32)
    dist = squares[:, None] + squares[None, :] - 2.0 * cross
    kernel_scale = 0.25 * D
    kernel = jnp.exp(-dist / kernel_scale)
    kernel_b = kernel.astype(jnp.bfloat16)
    rowsum = jnp.sum(kernel, axis=1)
    drive = jnp.dot(kernel_b, scores, preferred_element_type=jnp.float32)
    pull = jnp.dot(kernel_b, particles, preferred_element_type=jnp.float32)
    driving = drive / NP
    spreading = (particles_f * rowsum[:, None] - pull) / NP
    return driving, spreading
```

```python
import functools

import jax
import jax.numpy as jnp
from jax import lax
from jax.experimental import pallas as pl
from jax.experimental.pallas import tpu as pltpu
from jax.sharding import PartitionSpec as P

KERNEL_SCALE_PER_FEATURE = 0.25
PRIOR_PRECISION = 1.0
LANES = 128
CHUNKS = 4
PER_GROUP = 4
MIXED = 4
MESH = pl.DeviceIdType.MESH
BF16, F32 = jnp.bfloat16, jnp.float32
NT = (((1,), (1,)), ((), ()))


def ring_kernel(
    chips,
    p_hbm,
    d_hbm,
    labels,
    index,
    driving,
    spreading,
    rows,
    parts,
    mine,
    data,
    misfit,
    kern,
    sums,
    inbox,
    rowsum,
    rowsum_in,
    target_row,
    squares,
    local_sems,
    row_recv,
    row_send,
    row_sib_recv,
    row_sib_send,
    part_recv,
    part_send,
    mine_recv,
    mine_send,
    sums_recv,
    sums_send,
    rowsum_recv,
    rowsum_send,
):
    dom = lax.axis_index("dom")
    core = lax.rem(dom, 2)
    z = lax.div(dom, 2)
    right = lax.rem(z + 1, chips) * 2 + core
    left = lax.rem(z + chips - 1, chips) * 2 + core
    sibling = dom + 1 - 2 * core

    d = p_hbm.shape[1]
    np_own = p_hbm.shape[0]
    nb_own = index.shape[0]
    own_rows = d_hbm.shape[0]
    half = chips * nb_own
    nb = 2 * half
    wide = rows.shape[1]
    last = chips // 2
    groups = chips // PER_GROUP
    j_size = PER_GROUP * np_own
    total = float(2 * chips * np_own)
    ratio = float(own_rows) / float(nb_own)
    scale = KERNEL_SCALE_PER_FEATURE * d

    def slot_of(step, direction):
        return jnp.clip(2 * step - 1 + direction, 0, chips - 1)

    def row_chunk(slot, q):
        width = d // CHUNKS
        start = q * width
        if q == CHUNKS - 1:
            width += wide - d
        at = pl.multiple_of(slot * nb_own, nb_own)
        return rows.at[pl.ds(at, nb_own), pl.ds(start, width)]

    def part_chunk(slot, q):
        high, width = np_own // 2, d // 2
        at = pl.multiple_of(slot * np_own + (q // 2) * high, high)
        col = pl.multiple_of((q % 2) * width, width)
        return parts.at[pl.ds(at, high), pl.ds(col, width)]

    def hop(chunk, recv, send, step, direction, q):
        fixed = isinstance(step, int)
        src = 0 if fixed and step == 1 else slot_of(step - 1, direction)
        end = fixed and step == last
        return pltpu.make_async_remote_copy(
            src_ref=chunk(src, q),
            dst_ref=chunk(slot_of(step, direction), q),
            send_sem=send.at[2 * end + direction],
            recv_sem=recv.at[(direction * last + step - 1) * CHUNKS + q],
            device_id={"dom": right if direction == 0 else left},
            device_id_type=MESH,
        )

    row_hop = functools.partial(hop, row_chunk, row_recv, row_send)
    part_hop = functools.partial(hop, part_chunk, part_recv, part_send)

    def kept(direction, q):
        return q < CHUNKS // 2 if direction == 0 else q >= CHUNKS // 2

    def row_to_sibling(slot):
        at = pl.multiple_of(slot * nb_own, nb_own)
        return pltpu.make_async_remote_copy(
            src_ref=rows.at[pl.ds(at, nb_own), :],
            dst_ref=rows.at[pl.ds(half + at, nb_own), :],
            send_sem=row_sib_send,
            recv_sem=row_sib_recv,
            device_id={"dom": sibling},
            device_id_type=MESH,
        )

    load_data = pltpu.make_async_copy(d_hbm, data, local_sems.at[0])
    load_part = pltpu.make_async_copy(p_hbm, parts.at[pl.ds(0, np_own), :], local_sems.at[1])
    load_mine = pltpu.make_async_copy(p_hbm, mine.at[pl.ds(0, np_own), :], local_sems.at[2])
    load_part.start()
    load_data.start()
    load_mine.start()
    barrier = pltpu.get_barrier_semaphore()
    for peer in (left, right, sibling):
        pl.semaphore_signal(barrier, inc=1, device_id={"dom": peer}, device_id_type=MESH)

    load_part.wait()
    pl.semaphore_wait(barrier, 3)
    def part_mix(at):
        step, q = lax.div(at, CHUNKS), lax.rem(at, CHUNKS)

        @pl.when(step > 0)
        def _():
            for direction in (0, 1):
                part_hop(step, direction, q).wait_recv()

        for direction in (0, 1):
            part_hop(step + 1, direction, q).start()

    part_mix(jnp.int32(0))

    lane = lax.broadcasted_iota(jnp.int32, (nb_own, LANES), 1)
    sub = lax.broadcasted_iota(jnp.int32, (nb_own, LANES), 0)
    pick = jnp.zeros((nb_own, LANES), F32)
    target = jnp.zeros((nb_own, LANES), F32)
    for r in range(nb_own):
        at = lax.rem(index[r], own_rows)
        label = labels[at].astype(F32)
        pick = jnp.where((sub == r) & (lane == at), 1.0, pick)
        target = jnp.where((sub == r) & (lane == 0), label, target)
    load_data.wait()
    rows[pl.ds(0, nb_own), pl.ds(d, LANES)] = target.astype(BF16)
    rows[pl.ds(0, nb_own), pl.ds(0, d)] = jnp.dot(
        pick[:, :own_rows].astype(BF16), data[...], preferred_element_type=F32
    ).astype(BF16)

    for q in range(CHUNKS):
        row_hop(1, 0, q).start()
        row_hop(1, 1, q).start()
    swap = pltpu.make_async_remote_copy(
        src_ref=mine.at[pl.ds(0, np_own), :],
        dst_ref=mine.at[pl.ds(np_own, np_own), :],
        send_sem=mine_send,
        recv_sem=mine_recv,
        device_id={"dom": sibling},
        device_id_type=MESH,
    )
    row_to_sibling(0).start()
    load_mine.wait()
    swap.start()
    sums[...] = jnp.zeros_like(sums)
    rowsum[...] = jnp.zeros_like(rowsum)

    stride = CHUNKS // MIXED

    def mix_at(step):
        @pl.when(lax.rem(step, stride) == 0)
        def _():
            part_mix(lax.div(step, stride))

    def row_step(step, carry):
        for q in range(CHUNKS):
            for direction in (0, 1):
                row_hop(step, direction, q).wait_recv()
                row_hop(step + 1, direction, q).start()
        mix_at(step)
        row_to_sibling(2 * step - 1).start()
        row_to_sibling(2 * step).start()
        return carry

    lax.fori_loop(1, last - 1, row_step, 0)
    for q in range(CHUNKS):
        for direction in (0, 1):
            row_hop(last - 1, direction, q).wait_recv()
            if kept(direction, q):
                row_hop(last, direction, q).start()
    mix_at(jnp.int32(last - 1))
    row_to_sibling(2 * last - 3).start()
    row_to_sibling(2 * last - 2).start()
    for q in range(CHUNKS):
        row_hop(last, 0 if kept(0, q) else 1, q).wait_recv()
    row_to_sibling(chips - 1).start()
    lax.fori_loop((last - 1) // stride + 1, CHUNKS * (MIXED + 1), lambda at, c: (part_mix(at), c)[1], 0)
    swap.wait_recv()
    m = mine[...].astype(F32)
    squares[...] = jnp.broadcast_to(jnp.sum(m * m, axis=1, keepdims=True), squares.shape)
    pltpu.make_async_remote_copy(
        src_ref=rows.at[pl.ds(0, half), :],
        dst_ref=rows.at[pl.ds(half, half), :],
        send_sem=row_sib_send,
        recv_sem=row_sib_recv,
        device_id={"dom": sibling},
        device_id_type=MESH,
    ).wait()
    first = (lax.broadcasted_iota(jnp.int32, (8, LANES), 1) == 0).astype(BF16)
    target_row[...] = lax.dot_general(
        first, rows[:, pl.ds(d, LANES)], NT, preferred_element_type=F32
    )

    nbq, dq = nb // CHUNKS, d // CHUNKS

    def group_rows(group, many=1):
        return pl.ds(pl.multiple_of(group * j_size, j_size), many * j_size)

    def kernel_block(group, many=1):
        for i in range(many):
            block = parts[group_rows(group + i), :]
            cross = lax.dot_general(mine[...], block, NT, preferred_element_type=F32)
            folded = jnp.zeros((j_size, LANES), F32)
            for k in range(d // LANES):
                piece = parts[group_rows(group + i), pl.ds(k * LANES, LANES)].astype(F32)
                folded = folded + piece * piece
            others = jnp.sum(folded.T, axis=0, keepdims=True)
            dist = squares[:, :1] + others - 2.0 * cross
            kernel = jnp.exp(-dist / scale)
            kern[:, pl.ds(i * j_size, j_size)] = kernel.astype(BF16)
            rowsum[...] += kernel

    def misfit_block(group, q, many=1):
        logits = lax.dot_general(
            parts[group_rows(group, many), :],
            rows[pl.ds(q * nbq, nbq), pl.ds(0, d)],
            NT,
            preferred_element_type=F32,
        )
        misfit[pl.ds(0, many * j_size), pl.ds(q * nbq, nbq)] = (
            target_row[:1, pl.ds(q * nbq, nbq)] - jax.nn.sigmoid(logits)
        ).astype(BF16)

    def sums_block(group, q, many=1):
        cols = pl.ds(q * dq, dq)
        own = pl.ds(0, many * j_size)
        pulled = jnp.dot(misfit[own, :], rows[:, cols], preferred_element_type=F32)
        block = parts[group_rows(group, many), cols]
        scores = (-PRIOR_PRECISION * block.astype(F32) + ratio * pulled).astype(BF16)
        weights = kern[:, own]
        sums[0, :, cols] += jnp.dot(weights, scores, preferred_element_type=F32)
        sums[1, :, cols] += jnp.dot(weights, block, preferred_element_type=F32)

    ahead = MIXED // 2

    def part_step(group, carry):
        more = group < groups - 1
        double = group <= 2 * ahead - 2

        def work(block):
            pl.when(double)(lambda: block(2 * (group - ahead), 2))
            pl.when(jnp.logical_not(double))(lambda: block(group - 1, 1))

        for q in range(CHUNKS):
            step = 2 * group + 1
            for direction in (0, 1):
                part_hop(step, direction, q).wait_recv()
                if kept(direction, q):
                    part_hop(step + 1, direction, q).start()
                else:
                    pl.when(more)(part_hop(step + 1, direction, q).start)

            if q == 0:
                work(kernel_block)
            work(lambda at, many: misfit_block(at, q, many))

        for q in range(CHUNKS):
            step = 2 * group + 2
            for direction in (0, 1):

                def pass_on():
                    part_hop(step + 1, direction, q).start()

                if kept(direction, q):
                    part_hop(step, direction, q).wait_recv()
                    pl.when(more)(pass_on)
                else:

                    @pl.when(more)
                    def _():
                        part_hop(step, direction, q).wait_recv()
                        pass_on()

            work(lambda at, many: sums_block(at, q, many))

        return carry

    lax.fori_loop(ahead, groups, part_step, 0)

    def sums_hop(kind, q):
        cols = pl.ds(q * dq, dq)
        return pltpu.make_async_remote_copy(
            src_ref=sums.at[kind, pl.ds(np_own, np_own), cols],
            dst_ref=inbox.at[kind, :, cols],
            send_sem=sums_send.at[kind * CHUNKS + q],
            recv_sem=sums_recv.at[kind * CHUNKS + q],
            device_id={"dom": sibling},
            device_id_type=MESH,
        )

    rowsum_hop = pltpu.make_async_remote_copy(
        src_ref=rowsum.at[pl.ds(np_own, np_own), :],
        dst_ref=rowsum_in,
        send_sem=rowsum_send,
        recv_sem=rowsum_recv,
        device_id={"dom": sibling},
        device_id_type=MESH,
    )
    kernel_block(groups - 1)
    for q in range(CHUNKS):
        misfit_block(groups - 1, q)
        if q == 0:
            rowsum_hop.start()
    for q in range(CHUNKS):
        sums_block(groups - 1, q)
        if q > 0:
            sums_hop(0, q - 1).start()
            sums_hop(1, q - 1).start()
    rowsum_hop.wait_recv()
    own_rowsum = jnp.sum(
        rowsum[pl.ds(0, np_own), :] + rowsum_in[...], axis=1, keepdims=True
    )
    squares[pl.ds(0, np_own), :] = jnp.broadcast_to(own_rowsum, (np_own, LANES))
    sums_hop(0, CHUNKS - 1).start()
    sums_hop(1, CHUNKS - 1).start()
    for q in range(CHUNKS):
        cols = pl.ds(q * dq, dq)
        sums_hop(0, q).wait_recv()
        sums_hop(1, q).wait_recv()
        own = pl.ds(0, np_own)
        driving[:, cols] = (sums[0, own, cols] + inbox[0, :, cols]) / total
        pull = sums[1, own, cols] + inbox[1, :, cols]
        spreading[:, cols] = (mine[own, cols].astype(F32) * squares[own, :1] - pull) / total

    for q in range(CHUNKS):
        sums_hop(0, q).wait_send()
        sums_hop(1, q).wait_send()
    rowsum_hop.wait_send()
    swap.wait_send()
    for direction, peer in ((0, right), (1, left)):
        sent = (last - 1) * nb_own
        middle = d // 2
        cols = pl.ds(0, middle) if direction == 0 else pl.ds(middle, wide - middle)
        for end, region in enumerate(
            (rows.at[pl.ds(0, sent), :], rows.at[pl.ds(0, nb_own), cols])
        ):
            pltpu.make_async_remote_copy(
                src_ref=region,
                dst_ref=region,
                send_sem=row_send.at[2 * end + direction],
                recv_sem=row_recv.at[0],
                device_id={"dom": peer},
                device_id_type=MESH,
            ).wait_send()
        sent = (2 * last - 1) * np_own // 2
        pltpu.make_async_remote_copy(
            src_ref=parts.at[pl.ds(0, sent), :],
            dst_ref=parts.at[pl.ds(0, sent), :],
            send_sem=part_send.at[direction],
            recv_sem=part_recv.at[0],
            device_id={"dom": peer},
            device_id_type=MESH,
        ).wait_send()


def per_device(chips, particles, dataset, labels, batch_index):
    np_own, d = particles.shape
    nb_own = batch_index.shape[0]
    nb = 2 * chips * nb_own
    j_size = PER_GROUP * np_own
    hops = 2 * (chips // 2) * CHUNKS
    dma = pltpu.SemaphoreType.DMA
    out = jax.ShapeDtypeStruct((np_own, d), F32)
    return pl.pallas_call(
        functools.partial(ring_kernel, chips),
        out_shape=(out, out),
        in_specs=[
            pl.BlockSpec(memory_space=pl.ANY),
            pl.BlockSpec(memory_space=pl.ANY),
            pl.BlockSpec(memory_space=pltpu.SMEM),
            pl.BlockSpec(memory_space=pltpu.SMEM),
        ],
        out_specs=[pl.BlockSpec(memory_space=pltpu.VMEM)] * 2,
        scratch_shapes=[
            pltpu.VMEM((nb, d + LANES), BF16),
            pltpu.VMEM((chips * np_own, d), BF16),
            pltpu.VMEM((2 * np_own, d), BF16),
            pltpu.VMEM(dataset.shape, BF16),
            pltpu.VMEM((2 * j_size, nb), BF16),
            pltpu.VMEM((2 * np_own, 2 * j_size), BF16),
            pltpu.VMEM((2, 2 * np_own, d), F32),
            pltpu.VMEM((2, np_own, d), F32),
            pltpu.VMEM((2 * np_own, j_size), F32),
            pltpu.VMEM((np_own, j_size), F32),
            pltpu.VMEM((8, nb), F32),
            pltpu.VMEM((2 * np_own, LANES), F32),
            dma((3,)),
            dma((hops,)),
            dma((4,)),
            dma,
            dma,
            dma((hops,)),
            dma((2,)),
            dma,
            dma,
            dma((2 * CHUNKS,)),
            dma((2 * CHUNKS,)),
            dma,
            dma,
        ],
        compiler_params=pltpu.CompilerParams(collective_id=0, has_side_effects=True),
    )(particles, dataset, labels, batch_index)


def solution(mesh):
    placed = (
        P(("groups", "dom"), None),
        P(("groups", "dom"), None),
        P(("groups", "dom")),
        P(("groups", "dom")),
    )
    return jax.shard_map(
        functools.partial(per_device, mesh.shape["dom"] // 2),
        mesh=mesh,
        in_specs=placed,
        out_specs=(P(("groups", "dom"), None), P(("groups", "dom"), None)),
        check_vma=False,
    )
```
